16 devices in a mesh: dp: 4 (over y, z, core), tp: 4 (over x).
Axes of the slice: x: 4, y: 2, z: 1, core: 2. Of those that a mesh axis runs over, the one named last changes fastest.
The devices are a block of a 4x4x8 slice.
Arguments:
- x: bfloat16 [512, 3072], P('dp'), parts along dimension 0
- w_gate: bfloat16 [3072, 8192], P(None, 'tp')
- w_up: bfloat16 [3072, 8192], P(None, 'tp')
- w_down: bfloat16 [8192, 3072], P('tp')
Outputs:
- output: bfloat16 [512, 3072], P('dp'), parts along dimension 0
There are 4 independent parts. The reference program is written for one: setup_inputs(seed, part) draws one part's arguments, and reference() takes and returns one part's arrays. A program takes and returns all parts, laid end to end along the dimension named above; an argument that names none is the same for every part.
All inputs are finite; a program needn't handle non-finite values.
Results may differ from the reference program's by a relative error of at most 0.016.
Values are sent between devices in bfloat16 or wider.
A program may use at most 768 MiB of HBM per device.

```python
import jax
import jax.numpy as jnp

ROWS = 128
D = 3072
FF = 8192


def setup_inputs(seed: int = 0, part: int = 0) -> dict:
    kx, kg, ku, kd = jax.random.split(jax.random.key(seed), 4)
    drawn = {
        "x": jax.random.normal(jax.random.fold_in(kx, part), (ROWS, D), jnp.float32),
        "w_gate": jax.random.normal(kg, (D, FF), jnp.float32) * D**-0.5,
        "w_up": jax.random.normal(ku, (D, FF), jnp.float32) * D**-0.5,
        "w_down": jax.random.normal(kd, (FF, D), jnp.float32) * FF**-0.5,
    }
    return {k: v.astype(jnp.bfloat16) for k, v in drawn.items()}


def reference(x, w_gate, w_up, w_down):
    gate = jnp.dot(x, w_gate, preferred_element_type=jnp.float32)
    up = jnp.dot(x, w_up, preferred_element_type=jnp.float32)
    hidden = (jax.nn.silu(gate) * up).astype(jnp.bfloat16)
    return jnp.dot(hidden, w_down, preferred_element_type=jnp.float32).astype(jnp.bfloat16)
```

```python
import functools

import jax
import jax.numpy as jnp
from jax import lax
from jax.experimental import pallas as pl
from jax.experimental.pallas import tpu as pltpu
from jax.sharding import PartitionSpec as P

MESH = pl.DeviceIdType.MESH
BN = 256
BC = 256
RIGHT, LEFT = 0, 1


def kernel(
    tp,
    x_hbm, wg_hbm, wu_hbm, wd_hbm,
    out,
    xs, wg, wu, wd, hid, hsend, fsend, frecv, rsend, lsend, from_left, from_right, sterm, oterm,
    xsem, gsem, usem, dsem, xrem, hrem, fs, fr, ss, sr, os_, or_, gas, gar, gbs, gbr, hs, hr,
):
    rows, depth = x_hbm.shape
    top = rows // 2
    nj = wg.shape[0]
    fh = nj * BN
    chunk = depth // tp
    nb = chunk // BC

    me = lax.axis_index("tp")
    dp = lax.axis_index("dp")
    core = lax.rem(dp, 2)
    partner = dp + 1 - 2 * core
    right, left = lax.rem(me + 1, tp), lax.rem(me + tp - 1, tp)
    to_right, to_left, to_partner = {"tp": right}, {"tp": left}, {"dp": partner}

    x_copy = pltpu.make_async_copy(x_hbm, xs.at[0], xsem)
    x_copy.start()
    gate_copies, up_copies = [], []
    for j in range(nj):
        cols = pl.ds(pl.multiple_of(core * fh + j * BN, BN), BN)
        gate_copies.append(pltpu.make_async_copy(wg_hbm.at[:, cols], wg.at[j], gsem.at[j]))
        up_copies.append(pltpu.make_async_copy(wu_hbm.at[:, cols], wu.at[j], usem.at[j]))
        gate_copies[j].start()
        up_copies[j].start()
    order = [(2, b) for b in range(nb)] + [(r, b) for b in range(nb) for r in (1, 3)] + [(0, b) for b in range(nb)]
    slot = {key: s for s, key in enumerate(order)}

    def columns(r, b):
        return pl.ds(pl.multiple_of(lax.rem(me + r, tp) * chunk + b * BC, BC), BC)

    down_copies = []
    for s, (r, b) in enumerate(order):
        pair = []
        for half in range(2):
            units = pl.ds(pl.multiple_of(lax.rem(core + half, 2) * fh, fh), fh)
            pair.append(
                pltpu.make_async_copy(
                    wd_hbm.at[units, columns(r, b)], wd.at[s, pl.ds(half * fh, fh)], dsem.at[s, half]
                )
            )
            pair[half].start()
        down_copies.append(pair)

    barrier = pltpu.get_barrier_semaphore()
    for device in (to_partner, to_right, to_left):
        pl.semaphore_signal(barrier, inc=1, device_id=device, device_id_type=MESH)
    x_copy.wait()
    pl.semaphore_wait(barrier, 3)

    def remote(src, dst, send, recv, device):
        return pltpu.make_async_remote_copy(
            src_ref=src, dst_ref=dst, send_sem=send, recv_sem=recv, device_id=device, device_id_type=MESH
        )

    x_remote = remote(xs.at[0], xs.at[1], xrem.at[0], xrem.at[1], to_partner)
    x_remote.start()

    waited = set()
    hidden_remote = []

    def block(j, other):
        if j not in waited:
            waited.add(j)
            gate_copies[j].wait()
            up_copies[j].wait()
        x = xs[1 if other else 0]
        gate = jnp.dot(x, wg[j], preferred_element_type=jnp.float32)
        up = jnp.dot(x, wu[j], preferred_element_type=jnp.float32)
        h = (jax.nn.silu(gate) * up).astype(jnp.bfloat16)
        if not other:
            hid[:, pl.ds(j * BN, BN)] = h
            return
        hsend[j] = h
        copy = remote(hsend.at[j], hid.at[:, pl.ds(fh + j * BN, BN)], hrem.at[0, j], hrem.at[1, j], to_partner)
        copy.start()
        hidden_remote.append(copy)

    block(0, False)
    block(1, False)
    x_remote.wait_recv()
    for j in range(nj):
        block(j, True)
    for j in range(2, nj):
        block(j, False)
    for copy in hidden_remote:
        copy.wait_recv()

    def term(r, b):
        s = slot[r, b]
        down_copies[s][0].wait()
        down_copies[s][1].wait()
        return jnp.dot(hid[...], wd[s], preferred_element_type=jnp.float32)

    A, B = pl.ds(0, top), pl.ds(top, top)
    sides = ((RIGHT, A, to_right), (LEFT, B, to_left))
    sends = []

    def go(copy):
        copy.start()
        sends.append(copy)
        return copy

    f = {}
    for b in range(nb):
        fsend[b] = term(2, b).astype(jnp.bfloat16)
        for d, part, device in sides:
            f[b, d] = go(remote(fsend.at[b, part], frecv.at[b, part], fs.at[b, d], fr.at[b, d], device))

    o, s_ = {}, {}

    def neighbour_terms(b):
        t = term(1, b)
        rsend[b, B] = t[top:].astype(jnp.bfloat16)
        sterm[b, A] = t[:top]
        t = term(3, b)
        lsend[b, A] = t[:top].astype(jnp.bfloat16)
        sterm[b, B] = t[top:]

    def send_o(b):
        o[b, RIGHT] = go(remote(rsend.at[b, B], from_left.at[b, B], os_.at[b, RIGHT], or_.at[b, RIGHT], to_right))
        o[b, LEFT] = go(remote(lsend.at[b, A], from_right.at[b, A], os_.at[b, LEFT], or_.at[b, LEFT], to_left))

    def send_s(b):
        f[b, RIGHT].wait_recv()
        rsend[b, A] = (sterm[b, A] + frecv[b, A].astype(jnp.float32)).astype(jnp.bfloat16)
        s_[b, RIGHT] = go(remote(rsend.at[b, A], from_left.at[b, A], ss.at[b, RIGHT], sr.at[b, RIGHT], to_right))
        f[b, LEFT].wait_recv()
        lsend[b, B] = (sterm[b, B] + frecv[b, B].astype(jnp.float32)).astype(jnp.bfloat16)
        s_[b, LEFT] = go(remote(lsend.at[b, B], from_right.at[b, B], ss.at[b, LEFT], sr.at[b, LEFT], to_left))

    for b in range(nb):
        neighbour_terms(b)
        if b < nb - 1:
            send_o(b)
    for b in range(nb):
        send_s(b)
        if b == 0:
            send_o(nb - 1)
        oterm[b] = term(0, b)

    ga, gb = {}, {}

    def finish(b):
        for d in (RIGHT, LEFT):
            s_[b, d].wait_recv()
            o[b, d].wait_recv()
        total = oterm[b] + from_left[b].astype(jnp.float32) + from_right[b].astype(jnp.float32)
        out[:, columns(0, b)] = total.astype(jnp.bfloat16)

    def send_ga(b):
        for d, part, device in sides:
            piece = out.at[part, columns(0, b)]
            ga[b, d] = go(remote(piece, piece, gas.at[b, d], gar.at[b, d], device))

    def send_gb(b):
        for d, part, device in ((RIGHT, B, to_right), (LEFT, A, to_left)):
            piece = out.at[part, columns(0, b)]
            gb[b, d] = go(remote(piece, piece, gbs.at[b, d], gbr.at[b, d], device))

    h_ = {}

    def pass_on(b):
        for d, part, device, owner in ((RIGHT, A, to_right, tp - 1), (LEFT, B, to_left, 1)):
            ga[b, d].wait_recv()
            piece = out.at[part, columns(owner, b)]
            h_[b, d] = go(remote(piece, piece, hs.at[b, d], hr.at[b, d], device))

    for b in range(nb):
        finish(b)
        send_ga(b)
        if b < nb - 1:
            send_gb(b)
    for b in range(nb):
        pass_on(b)
        if b == 0:
            send_gb(nb - 1)
    for b in range(nb):
        for d in (RIGHT, LEFT):
            gb[b, d].wait_recv()
            h_[b, d].wait_recv()
    x_remote.wait_send()
    for copy in hidden_remote:
        copy.wait_send()
    for copy in sends:
        copy.wait_send()


def solution(mesh):
    tp = mesh.shape["tp"]

    def step(x, w_gate, w_up, w_down):
        rows, depth = x.shape
        units = w_gate.shape[1]
        nj = units // 2 // BN
        nb = depth // tp // BC
        bf16, f32 = jnp.bfloat16, jnp.float32
        pieces = pltpu.VMEM((nb, rows, BC), bf16)
        dma = pltpu.SemaphoreType.DMA
        two = dma((nb, 2))
        return pl.pallas_call(
            functools.partial(kernel, tp),
            out_shape=jax.ShapeDtypeStruct((rows, depth), bf16),
            in_specs=[pl.BlockSpec(memory_space=pltpu.HBM)] * 4,
            out_specs=pl.BlockSpec(memory_space=pltpu.VMEM),
            scratch_shapes=[
                pltpu.VMEM((2, rows, depth), bf16),
                pltpu.VMEM((nj, depth, BN), bf16),
                pltpu.VMEM((nj, depth, BN), bf16),
                pltpu.VMEM((tp * nb, units, BC), bf16),
                pltpu.VMEM((rows, units), bf16),
                pltpu.VMEM((nj, rows, BN), bf16),
                pieces, pieces, pieces, pieces, pieces, pieces,
                pltpu.VMEM((nb, rows, BC), f32),
                pltpu.VMEM((nb, rows, BC), f32),
                dma, dma((nj,)), dma((nj,)), dma((tp * nb, 2)), dma((2,)), dma((2, nj)),
                two, two, two, two, two, two, two, two, two, two, two, two,
            ],
            compiler_params=pltpu.CompilerParams(collective_id=0, has_side_effects=True),
        )(x, w_gate, w_up, w_down)

    return jax.shard_map(
        step,
        mesh=mesh,
        in_specs=(P("dp", None), P(None, "tp"), P(None, "tp"), P("tp", None)),
        out_specs=P("dp", None),
        check_vma=False,
    )
```

```python
import functools

import jax
import jax.numpy as jnp
from jax import lax
from jax.experimental import pallas as pl
from jax.experimental.pallas import tpu as pltpu
from jax.sharding import PartitionSpec as P

MESH = pl.DeviceIdType.MESH
BN = 256
BC = 256
RIGHT, LEFT = 0, 1


def kernel(
    tp,
    x_hbm, wg_hbm, wu_hbm, wd_hbm,
    out,
    xs, wg, wu, wd, hid, hsend, fsend, frecv, rsend, lsend, from_left, from_right, sterm, oterm,
    xsem, gsem, usem, dsem, xrem, hrem, fs, fr, ss, sr, os_, or_, gas, gar, gbs, gbr, hs, hr,
):
    rows, depth = x_hbm.shape
    top = rows // 2
    nj = wg.shape[0]
    fh = nj * BN
    chunk = depth // tp
    nb = chunk // BC

    me = lax.axis_index("tp")
    dp = lax.axis_index("dp")
    core = lax.rem(dp, 2)
    partner = dp + 1 - 2 * core
    right, left = lax.rem(me + 1, tp), lax.rem(me + tp - 1, tp)
    to_right, to_left, to_partner = {"tp": right}, {"tp": left}, {"dp": partner}

    x_copy = pltpu.make_async_copy(x_hbm, xs.at[0], xsem)
    gate_copies, up_copies = [], []
    for j in range(nj):
        cols = pl.ds(pl.multiple_of(core * fh + j * BN, BN), BN)
        gate_copies.append(pltpu.make_async_copy(wg_hbm.at[:, cols], wg.at[j], gsem.at[j]))
        up_copies.append(pltpu.make_async_copy(wu_hbm.at[:, cols], wu.at[j], usem.at[j]))

    def columns(r, start, size):
        return pl.ds(pl.multiple_of(lax.rem(me + r, tp) * chunk + start, BC), size)

    down_copies = []
    for i, (r, start, size) in enumerate(((2, 0, BC), (2, BC, chunk - BC), (1, 0, chunk), (3, 0, chunk), (0, 0, chunk))):
        down_copies.append(
            pltpu.make_async_copy(
                wd_hbm.at[:, columns(r, start, size)], wd.at[r, :, pl.ds(start, size)], dsem.at[i]
            )
        )
    pending = [x_copy] + [c for j in range(nj) for c in (gate_copies[j], up_copies[j])] + down_copies

    def wait_read(copy):
        copy.wait()
        if pending:
            pending.pop(0).start()

    for _ in range(3):
        pending.pop(0).start()

    barrier = pltpu.get_barrier_semaphore()
    for device in (to_partner, to_right, to_left):
        pl.semaphore_signal(barrier, inc=1, device_id=device, device_id_type=MESH)
    with jax.named_scope('x_wait'):
        wait_read(x_copy)
    with jax.named_scope('barrier'):
        pl.semaphore_wait(barrier, 3)

    def remote(src, dst, send, recv, device):
        return pltpu.make_async_remote_copy(
            src_ref=src, dst_ref=dst, send_sem=send, recv_sem=recv, device_id=device, device_id_type=MESH
        )

    x_remote = remote(xs.at[0], xs.at[1], xrem.at[0], xrem.at[1], to_partner)
    x_remote.start()

    waited = set()
    hidden_remote = []

    def block(j, other):
        if j not in waited:
            waited.add(j)
            wait_read(gate_copies[j])
            wait_read(up_copies[j])
        x = xs[1 if other else 0]
        units = pl.ds(pl.multiple_of(core * fh + j * BN, BN), BN)
        gate = jnp.dot(x, wg[j], preferred_element_type=jnp.float32)
        up = jnp.dot(x, wu[j], preferred_element_type=jnp.float32)
        h = (jax.nn.silu(gate) * up).astype(jnp.bfloat16)
        if not other:
            hid[:, units] = h
            return
        hsend[j] = h
        copy = remote(hsend.at[j], hid.at[:, units], hrem.at[0, j], hrem.at[1, j], to_partner)
        copy.start()
        hidden_remote.append(copy)

    with jax.named_scope("own01"):
        block(0, False)
        block(1, False)
    with jax.named_scope("x_remote"):
        x_remote.wait_recv()
    with jax.named_scope("other"):
        for j in range(nj):
            block(j, True)
    with jax.named_scope("own23"):
        for j in range(2, nj):
            block(j, False)
    with jax.named_scope("hidden_remote"):
        for copy in hidden_remote:
            copy.wait_recv()

    def terms(*keys):
        out = []
        for r, b in keys:
            w = wd.at[r, :, pl.ds(b * BC, BC)]
            out.append(
                jnp.dot(hid[:, :fh], w[:fh], preferred_element_type=jnp.float32)
                + jnp.dot(hid[:, fh:], w[fh:], preferred_element_type=jnp.float32)
            )
        return out

    A, B = pl.ds(0, top), pl.ds(top, top)
    sides = ((RIGHT, A, to_right), (LEFT, B, to_left))
    sends = []

    def go(copy):
        copy.start()
        sends.append(copy)
        return copy

    f = {}

    def send_f(b):
        for d, part, device in sides:
            f[b, d] = go(remote(fsend.at[b, part], frecv.at[b, part], fs.at[b, d], fr.at[b, d], device))

    with jax.named_scope("f0"):
        wait_read(down_copies[0])
        fsend[0] = terms((2, 0))[0].astype(jnp.bfloat16)
        send_f(0)
    with jax.named_scope("f12"):
        wait_read(down_copies[1])
        for b, t in zip(range(1, nb), terms(*((2, b) for b in range(1, nb)))):
            fsend[b] = t.astype(jnp.bfloat16)
            send_f(b)

    o, s_ = {}, {}

    def neighbour_terms(b):
        t, u = terms((1, b), (3, b))
        rsend[b, B] = t[top:].astype(jnp.bfloat16)
        sterm[b, A] = t[:top]
        lsend[b, A] = u[:top].astype(jnp.bfloat16)
        sterm[b, B] = u[top:]

    def send_o(b):
        o[b, RIGHT] = go(remote(rsend.at[b, B], from_left.at[b, B], os_.at[b, RIGHT], or_.at[b, RIGHT], to_right))
        o[b, LEFT] = go(remote(lsend.at[b, A], from_right.at[b, A], os_.at[b, LEFT], or_.at[b, LEFT], to_left))

    def send_s(b):
        f[b, RIGHT].wait_recv()
        rsend[b, A] = (sterm[b, A] + frecv[b, A].astype(jnp.float32)).astype(jnp.bfloat16)
        s_[b, RIGHT] = go(remote(rsend.at[b, A], from_left.at[b, A], ss.at[b, RIGHT], sr.at[b, RIGHT], to_right))
        f[b, LEFT].wait_recv()
        lsend[b, B] = (sterm[b, B] + frecv[b, B].astype(jnp.float32)).astype(jnp.bfloat16)
        s_[b, LEFT] = go(remote(lsend.at[b, B], from_right.at[b, B], ss.at[b, LEFT], sr.at[b, LEFT], to_left))

    for b in range(nb):
        with jax.named_scope(f"neighbour{b}"):
            if b == 0:
                wait_read(down_copies[2])
                wait_read(down_copies[3])
            neighbour_terms(b)
            if b < nb - 1:
                send_o(b)
    with jax.named_scope("own_terms"):
        wait_read(down_copies[4])
        for b, t in enumerate(terms(*((0, b) for b in range(nb)))):
            oterm[b] = t
    for b in range(nb):
        with jax.named_scope(f"s{b}"):
            send_s(b)
            if b == 0:
                send_o(nb - 1)

    ga, gb = {}, {}

    def finish(b):
        for d in (RIGHT, LEFT):
            s_[b, d].wait_recv()
            o[b, d].wait_recv()
        total = oterm[b] + from_left[b].astype(jnp.float32) + from_right[b].astype(jnp.float32)
        out[:, columns(0, b * BC, BC)] = total.astype(jnp.bfloat16)

    def send_ga(b):
        for d, part, device in sides:
            piece = out.at[part, columns(0, b * BC, BC)]
            ga[b, d] = go(remote(piece, piece, gas.at[b, d], gar.at[b, d], device))

    def send_gb(b):
        for d, part, device in ((RIGHT, B, to_right), (LEFT, A, to_left)):
            piece = out.at[part, columns(0, b * BC, BC)]
            gb[b, d] = go(remote(piece, piece, gbs.at[b, d], gbr.at[b, d], device))

    h_ = {}

    def pass_on(b):
        for d, part, device, owner in ((RIGHT, A, to_right, tp - 1), (LEFT, B, to_left, 1)):
            ga[b, d].wait_recv()
            piece = out.at[part, columns(owner, b * BC, BC)]
            h_[b, d] = go(remote(piece, piece, hs.at[b, d], hr.at[b, d], device))

    finish_order = ["GA0", "GB0", "GA1", "GA2", "GB1", "H0", "GB2", "H1", "H2"]
    for step in finish_order:
        kind, b = step[:-1], int(step[-1])
        with jax.named_scope(step):
            if kind == "GA":
                finish(b)
                send_ga(b)
            elif kind == "GB":
                send_gb(b)
            else:
                pass_on(b)
    with jax.named_scope("last"):
        for b in range(nb):
            for d in (RIGHT, LEFT):
                gb[b, d].wait_recv()
                h_[b, d].wait_recv()
    with jax.named_scope("drain"):
        x_remote.wait_send()
        for copy in hidden_remote:
            copy.wait_send()
        for copy in sends:
            copy.wait_send()


def solution(mesh):
    tp = mesh.shape["tp"]

    def step(x, w_gate, w_up, w_down):
        rows, depth = x.shape
        units = w_gate.shape[1]
        nj = units // 2 // BN
        nb = depth // tp // BC
        bf16, f32 = jnp.bfloat16, jnp.float32
        pieces = pltpu.VMEM((nb, rows, BC), bf16)
        dma = pltpu.SemaphoreType.DMA
        two = dma((nb, 2))
        return pl.pallas_call(
            functools.partial(kernel, tp),
            out_shape=jax.ShapeDtypeStruct((rows, depth), bf16),
            in_specs=[pl.BlockSpec(memory_space=pltpu.HBM)] * 4,
            out_specs=pl.BlockSpec(memory_space=pltpu.VMEM),
            scratch_shapes=[
                pltpu.VMEM((2, rows, depth), bf16),
                pltpu.VMEM((nj, depth, BN), bf16),
                pltpu.VMEM((nj, depth, BN), bf16),
                pltpu.VMEM((tp, units, depth // tp), bf16),
                pltpu.VMEM((rows, units), bf16),
                pltpu.VMEM((nj, rows, BN), bf16),
                pieces, pieces, pieces, pieces, pieces, pieces,
                pltpu.VMEM((nb, rows, BC), f32),
                pltpu.VMEM((nb, rows, BC), f32),
                dma, dma((nj,)), dma((nj,)), dma((5,)), dma((2,)), dma((2, nj)),
                two, two, two, two, two, two, two, two, two, two, two, two,
            ],
            compiler_params=pltpu.CompilerParams(
                collective_id=0, has_side_effects=True, vmem_limit_bytes=40 * 2**20
            ),
        )(*(pltpu.with_memory_space_constraint(a, pltpu.HBM) for a in (x, w_gate, w_up, w_down)))

    return jax.shard_map(
        step,
        mesh=mesh,
        in_specs=(P("dp", None), P(None, "tp"), P(None, "tp"), P("tp", None)),
        out_specs=P("dp", None),
        check_vma=False,
    )
```

```python
import functools

import jax
import jax.numpy as jnp
from jax import lax
from jax.experimental import pallas as pl
from jax.experimental.pallas import tpu as pltpu
from jax.sharding import PartitionSpec as P

MESH = pl.DeviceIdType.MESH
BN = 256
BC = 256
UNIT = 128
BATCHES = ((0, 1), (1, 1), (2, 1), (3, 1), (4, 2))
FIRST0 = ('g0', 'r4', 'm0', 'x0', 'p0', 'g1', 'r2', 'm1p1', 'g2', 'r1', 'h0', 'h1', 'p2', 'g3', 'h2', 'p3', 'h3', 'r1', 'm2m3')
FIRST1 = ('g0', 'r4', 'm0', 'g1', 'r2', 'm1', 'x0', 'p0p1', 'g2', 'r1', 'h0', 'h1', 'p2', 'g3', 'h2', 'p3', 'h3', 'r1', 'm2m3')
PLAN0 = ('c0', 'F2', 'c1', 'F4', 'F1', 'F3', 'F0', 'c2', 'O1', 'c3', 'O3', 'c4', 'O4', 'O2', 'S2', 'S4', 'O0', 'c5', 'S1', 'S3', 'S0', 'P2', 'Q2', 'P4', 'P1', 'P3', 'P0', 'Q1', 'Q0', 'Q3', 'H2', 'Q4', 'H4', 'H1', 'H3', 'H0')
PLAN1 = ('c0', 'F2', 'F0', 'F3', 'c1', 'c2', 'O0', 'c3', 'F4', 'S0', 'S2', 'F1', 'O2', 'c4', 'c5', 'O3', 'S3', 'P0', 'O4', 'S4', 'O1', 'Q0', 'P2', 'Q2', 'S1', 'P3', 'Q3', 'P4', 'H0', 'P1', 'Q1', 'Q4', 'H3', 'H2', 'H1', 'H4')


def kernel(
    tp,
    x_hbm, wg_hbm, wu_hbm, wd_hbm,
    out,
    xs, wgu, wd, hid, hsend, fsend, frecv, rsend, lsend, beside, sterm, oterm,
    reads, downs, far, arrived, sent,
):
    rows, depth = x_hbm.shape
    top = rows // 2
    nj = wgu.shape[0]
    fh = nj * BN
    chunk = depth // tp
    nb = chunk // BC
    nbatch = len(BATCHES)
    bf16, f32 = jnp.bfloat16, jnp.float32

    me = lax.axis_index("tp")
    dp = lax.axis_index("dp")
    core = lax.rem(dp, 2)
    partner = dp + 1 - 2 * core
    right, left = lax.rem(me + 1, tp), lax.rem(me + tp - 1, tp)
    to_right, to_left, to_partner = {"tp": right}, {"tp": left}, {"dp": partner}

    barrier = pltpu.get_barrier_semaphore()
    even = lax.rem(me, 2) == 0

    def greet(*devices):
        for device in devices:
            pl.semaphore_signal(barrier, inc=1, device_id=device, device_id_type=MESH)

    greet(to_partner)

    def remote(src, dst, send, recv, device):
        return pltpu.make_async_remote_copy(
            src_ref=src, dst_ref=dst, send_sem=send, recv_sem=recv, device_id=device, device_id_type=MESH
        )

    def wait(ref, sem):
        pltpu.make_async_copy(ref, ref, sem).wait()

    def units(j):
        return pl.ds(pl.multiple_of(core * fh + j * BN, BN), BN)

    def columns(r, start, size):
        return pl.ds(pl.multiple_of(lax.rem(me + r, tp) * chunk + start, UNIT), size)

    pending = [pltpu.make_async_copy(x_hbm, xs.at[0], reads.at[nj])]
    for j in range(nj):
        for i, w in enumerate((wg_hbm, wu_hbm)):
            pending.append(pltpu.make_async_copy(w.at[:, units(j)], wgu.at[j, i], reads.at[j]))
    downs_of = ((2, 0, 2 * BC), (2, 2 * BC, chunk - 2 * BC), (1, 0, chunk), (3, 0, chunk), (0, 0, chunk))
    for i, (r, start, size) in enumerate(downs_of):
        pending.append(
            pltpu.make_async_copy(wd_hbm.at[:, columns(r, start, size)], wd.at[r, :, pl.ds(start, size)], downs.at[i])
        )
    down_copies = pending[-len(downs_of) :]

    def start_reads(count):
        for _ in range(count):
            pending.pop(0).start()

    start_reads(3)
    with jax.named_scope("barrier"):
        pl.when(even)(lambda: pl.semaphore_wait(barrier, 1))
        pl.when(jnp.logical_not(even))(lambda: pl.semaphore_wait(barrier, 3))
        greet(to_right, to_left)
    with jax.named_scope("x_wait"):
        wait(xs.at[0], reads.at[nj])
        start_reads(2)
    x_remote = remote(xs.at[0], xs.at[1], far.at[0], far.at[1], to_partner)
    x_remote.start()

    def block(j, other):
        x = xs[1 if other else 0]
        gate = jnp.dot(x, wgu[j, 0], preferred_element_type=f32)
        up = jnp.dot(x, wgu[j, 1], preferred_element_type=f32)
        h = (jax.nn.silu(gate) * up).astype(bf16)
        if other:
            hsend[:, pl.ds(j * BN, BN)] = h
        else:
            hid[:, units(j)] = h

    def hidden(plan, later):
        for word in plan:
            with jax.named_scope(word):
                kind, j = word[0], int(word[1])
                if kind == "g":
                    wait(wgu.at[j], reads.at[j])
                elif kind == "x":
                    x_remote.wait_recv()
                elif kind == "h":
                    remote(
                        hsend.at[:, pl.ds(j * BN, BN)], hid.at[:, units(j)], far.at[2], far.at[3], to_partner
                    ).start()
                elif kind == "r":
                    for _ in range(j):
                        later.pop(0).start()
                else:
                    for i in range(0, len(word), 2):
                        block(int(word[i + 1]), word[i] == "p")
        with jax.named_scope("hidden_remote"):
            wait(hid.at[:, pl.ds(pl.multiple_of((1 - core) * fh, fh), fh)], far.at[3])
            pl.when(even)(lambda: pl.semaphore_wait(barrier, 2))

    A, B = pl.ds(0, top), pl.ds(top, top)
    sides = ((A, to_right), (B, to_left))
    others = ((B, to_right), (A, to_left))
    batches = [(UNIT * a, UNIT * n) for a, n in BATCHES]
    cols = [pl.ds(start, size) for start, size in batches]
    pieces = [(2, b) for b in range(nb)] + [(r, b) for b in range(nb) for r in (1, 3)] + [(0, b) for b in range(nb)]
    needs = {(2, 0): 0, (2, 2): 1, (1, 0): 2, (3, 0): 3, (0, 0): 4}

    def compute(i):
        pair = pieces[2 * i : 2 * i + 2]
        for key in pair:
            if key in needs:
                down_copies[needs[key]].wait()
                if needs[key] == 0:
                    down_copies[4].start()
        terms = [
            jnp.dot(hid[...], wd[r, :, pl.ds(b * BC, BC)], preferred_element_type=f32) for r, b in pair
        ]
        for (r, b), t in zip(pair, terms):
            at = pl.ds(b * BC, BC)
            if r == 2:
                fsend[:, at] = t.astype(bf16)
            elif r == 1:
                rsend[B, at] = t[top:].astype(bf16)
                sterm[A, at] = t[:top]
            elif r == 3:
                lsend[A, at] = t[:top].astype(bf16)
                sterm[B, at] = t[top:]
            else:
                oterm[:, at] = t

    def exchange(plan):
        def go(src, dst, which, device):
            remote(src, dst, sent, arrived.at[which], device).start()

        def out_piece(owner, b, part):
            return out.at[part, columns(owner, *batches[b])]

        def step(kind, b):
            if kind == "c":
                compute(b)
            elif kind == "F":
                for part, device in sides:
                    go(fsend.at[part, cols[b]], frecv.at[part, cols[b]], b, device)
            elif kind == "O":
                go(rsend.at[B, cols[b]], beside.at[0, B, cols[b]], nbatch + b, to_right)
                go(lsend.at[A, cols[b]], beside.at[1, A, cols[b]], nbatch + b, to_left)
            elif kind == "S":
                wait(frecv.at[:, cols[b]], arrived.at[b])
                total = (sterm[:, cols[b]] + frecv[:, cols[b]].astype(f32)).astype(bf16)
                rsend[A, cols[b]] = total[:top]
                lsend[B, cols[b]] = total[top:]
                go(rsend.at[A, cols[b]], beside.at[0, A, cols[b]], nbatch + b, to_right)
                go(lsend.at[B, cols[b]], beside.at[1, B, cols[b]], nbatch + b, to_left)
            elif kind == "P":
                wait(beside.at[:, :, cols[b]], arrived.at[nbatch + b])
                total = oterm[:, cols[b]] + beside[0, :, cols[b]].astype(f32) + beside[1, :, cols[b]].astype(f32)
                out[:, columns(0, *batches[b])] = total.astype(bf16)
                for part, device in sides:
                    go(out_piece(0, b, part), out_piece(0, b, part), 2 * nbatch + b, device)
            elif kind == "Q":
                for part, device in others:
                    go(out_piece(0, b, part), out_piece(0, b, part), 3 * nbatch, device)
            else:
                wait(frecv.at[:, cols[b]], arrived.at[2 * nbatch + b])
                for (part, device), owner in zip(sides, (tp - 1, 1)):
                    go(out_piece(owner, b, part), out_piece(owner, b, part), 3 * nbatch, device)

        for word in plan:
            with jax.named_scope(word):
                step(word[0], int(word[1:]))

    def run(first, plan):
        hidden(first, list(pending))
        exchange(plan)

    pl.when(core == 0)(lambda: run(FIRST0, PLAN0))
    pl.when(core == 1)(lambda: run(FIRST1, PLAN1))
    with jax.named_scope("last"):
        wait(beside, arrived.at[3 * nbatch])
    with jax.named_scope("drain"):
        x_remote.wait_send()
        wait(hsend, far.at[2])
        wait(wd.at[0, pl.ds(0, 6 * rows)], sent)


def solution(mesh):
    tp = mesh.shape["tp"]

    def step(x, w_gate, w_up, w_down):
        rows, depth = x.shape
        units = w_gate.shape[1]
        nj = units // 2 // BN
        chunk = depth // tp
        bf16, f32 = jnp.bfloat16, jnp.float32
        quarter = pltpu.VMEM((rows, chunk), bf16)
        dma = pltpu.SemaphoreType.DMA
        operands = [pltpu.with_memory_space_constraint(a, pltpu.HBM) for a in (x, w_gate, w_up, w_down)]
        return pl.pallas_call(
            functools.partial(kernel, tp),
            out_shape=jax.ShapeDtypeStruct((rows, depth), bf16),
            in_specs=[pl.BlockSpec(memory_space=pltpu.HBM)] * 4,
            out_specs=pl.BlockSpec(memory_space=pltpu.VMEM),
            scratch_shapes=[
                pltpu.VMEM((2, rows, depth), bf16),
                pltpu.VMEM((nj, 2, depth, BN), bf16),
                pltpu.VMEM((tp, units, chunk), bf16),
                pltpu.VMEM((rows, units), bf16),
                pltpu.VMEM((rows, units // 2), bf16),
                quarter, quarter, quarter, quarter,
                pltpu.VMEM((2, rows, chunk), bf16),
                pltpu.VMEM((rows, chunk), f32),
                pltpu.VMEM((rows, chunk), f32),
                dma((nj + 1,)), dma((5,)), dma((4,)), dma((3 * len(BATCHES) + 1,)), dma,
            ],
            compiler_params=pltpu.CompilerParams(
                collective_id=0, has_side_effects=True, vmem_limit_bytes=40 * 2**20
            ),
        )(*operands)

    return jax.shard_map(
        step,
        mesh=mesh,
        in_specs=(P("dp", None), P(None, "tp"), P(None, "tp"), P("tp", None)),
        out_specs=P("dp", None),
        check_vma=False,
    )
```

```python
import functools

import jax
import jax.numpy as jnp
from jax import lax
from jax.experimental import pallas as pl
from jax.experimental.pallas import tpu as pltpu
from jax.sharding import PartitionSpec as P

MESH = pl.DeviceIdType.MESH
BN = 256
BC = 256
UNIT = 128
BATCHES = ((0, 1), (1, 1), (2, 1), (3, 1), (4, 2))
FIRST0 = ('g0', 'r4', 'm0', 'x0', 'p0', 'g1', 'r2', 'm1p1', 'g2', 'r1', 'h0', 'h1', 'p2', 'g3', 'h2', 'p3', 'h3', 'r1', 'm2m3')
FIRST1 = ('g0', 'r4', 'm0', 'g1', 'r2', 'm1', 'x0', 'p0p1', 'g2', 'r1', 'h0', 'h1', 'p2', 'g3', 'h2', 'p3', 'h3', 'r1', 'm2m3')
PLAN0 = ('c0', 'F0', 'F1', 'c1', 'F2', 'F4', 'F3', 'c2', 'c3', 'c4', 'O2', 'O0', 'O4', 'c5', 'S0', 'S2', 'S4', 'S1', 'O1', 'S3', 'O3', 'P0', 'P2', 'Q2', 'P4', 'P1', 'Q0', 'P3', 'Q3', 'Q4', 'H2', 'Q1', 'H4', 'H0', 'H1', 'H3')
PLAN1 = ('c0', 'F1', 'F0', 'c1', 'c2', 'F2', 'F4', 'c3', 'O2', 'F3', 'O1', 'S1', 'c4', 'O0', 'O3', 'S0', 'c5', 'S2', 'P1', 'S4', 'O4', 'S3', 'Q1', 'P0', 'P2', 'Q0', 'P4', 'P3', 'Q4', 'Q2', 'H0', 'H1', 'H2', 'Q3', 'H4', 'H3')


def kernel(
    tp,
    x_hbm, wg_hbm, wu_hbm, wd_hbm,
    out,
    xs, wgu, wd, hid, hsend, fsend, frecv, rsend, lsend, beside, sterm, oterm,
    reads, downs, far, arrived, sent,
):
    rows, depth = x_hbm.shape
    top = rows // 2
    nj = wgu.shape[0]
    fh = nj * BN
    chunk = depth // tp
    nb = chunk // BC
    nbatch = len(BATCHES)
    bf16, f32 = jnp.bfloat16, jnp.float32

    me = lax.axis_index("tp")
    dp = lax.axis_index("dp")
    core = lax.rem(dp, 2)
    partner = dp + 1 - 2 * core
    right, left = lax.rem(me + 1, tp), lax.rem(me + tp - 1, tp)
    to_right, to_left, to_partner = {"tp": right}, {"tp": left}, {"dp": partner}

    barrier = pltpu.get_barrier_semaphore()
    even = lax.rem(me, 2) == 0

    def greet(*devices):
        for device in devices:
            pl.semaphore_signal(barrier, inc=1, device_id=device, device_id_type=MESH)

    greet(to_partner)

    def remote(src, dst, send, recv, device):
        return pltpu.make_async_remote_copy(
            src_ref=src, dst_ref=dst, send_sem=send, recv_sem=recv, device_id=device, device_id_type=MESH
        )

    def wait(ref, sem):
        pltpu.make_async_copy(ref, ref, sem).wait()

    def units(j):
        return pl.ds(pl.multiple_of(core * fh + j * BN, BN), BN)

    def columns(r, start, size):
        return pl.ds(pl.multiple_of(lax.rem(me + r, tp) * chunk + start, UNIT), size)

    pending = [pltpu.make_async_copy(x_hbm, xs.at[0], reads.at[nj])]
    for j in range(nj):
        for i, w in enumerate((wg_hbm, wu_hbm)):
            pending.append(pltpu.make_async_copy(w.at[:, units(j)], wgu.at[j, i], reads.at[j]))
    downs_of = ((2, 0, 2 * BC), (2, 2 * BC, chunk - 2 * BC), (1, 0, chunk), (3, 0, chunk), (0, 0, chunk))
    for i, (r, start, size) in enumerate(downs_of):
        pending.append(
            pltpu.make_async_copy(wd_hbm.at[:, columns(r, start, size)], wd.at[r, :, pl.ds(start, size)], downs.at[i])
        )
    down_copies = pending[-len(downs_of) :]

    def start_reads(count):
        for _ in range(count):
            pending.pop(0).start()

    start_reads(3)
    with jax.named_scope("barrier"):
        pl.when(even)(lambda: pl.semaphore_wait(barrier, 1))
        pl.when(jnp.logical_not(even))(lambda: pl.semaphore_wait(barrier, 3))
        greet(to_right, to_left)
    with jax.named_scope("x_wait"):
        wait(xs.at[0], reads.at[nj])
        start_reads(2)
    x_remote = remote(xs.at[0], xs.at[1], far.at[0], far.at[1], to_partner)
    x_remote.start()

    def block(j, other):
        x = xs[1 if other else 0]
        gate = jnp.dot(x, wgu[j, 0], preferred_element_type=f32)
        up = jnp.dot(x, wgu[j, 1], preferred_element_type=f32)
        h = (jax.nn.silu(gate) * up).astype(bf16)
        if other:
            hsend[:, pl.ds(j * BN, BN)] = h
        else:
            hid[:, units(j)] = h

    def hidden(plan, later):
        for word in plan:
            with jax.named_scope(word):
                kind, j = word[0], int(word[1])
                if kind == "g":
                    wait(wgu.at[j], reads.at[j])
                elif kind == "x":
                    x_remote.wait_recv()
                elif kind == "h":
                    remote(
                        hsend.at[:, pl.ds(j * BN, BN)], hid.at[:, units(j)], far.at[2], far.at[3], to_partner
                    ).start()
                elif kind == "r":
                    for _ in range(j):
                        later.pop(0).start()
                else:
                    for i in range(0, len(word), 2):
                        block(int(word[i + 1]), word[i] == "p")
        with jax.named_scope("hidden_remote"):
            wait(hid.at[:, pl.ds(pl.multiple_of((1 - core) * fh, fh), fh)], far.at[3])
            pl.when(even)(lambda: pl.semaphore_wait(barrier, 2))

    A, B = pl.ds(0, top), pl.ds(top, top)
    sides = ((A, to_right), (B, to_left))
    others = ((B, to_right), (A, to_left))
    batches = [(UNIT * a, UNIT * n) for a, n in BATCHES]
    cols = [pl.ds(start, size) for start, size in batches]
    steps = [[(2, 0)], [(2, b) for b in range(1, nb)]] + [[(1, b), (3, b)] for b in range(nb)] + [[(0, b) for b in range(nb)]]
    needs = {(2, 0): 0, (2, 2): 1, (1, 0): 2, (3, 0): 3, (0, 0): 4}

    def compute(i):
        pair = steps[i]
        for key in pair:
            if key in needs:
                down_copies[needs[key]].wait()
                if needs[key] == 0:
                    down_copies[4].start()
        def product(r, b, half, sign):
            return jnp.dot(sign * hid[:, half], wd[r, half, pl.ds(b * BC, BC)], preferred_element_type=f32)

        if len(pair) == 1:
            terms = [product(*pair[0], pl.ds(0, fh), 1) - product(*pair[0], pl.ds(fh, fh), -1)]
        else:
            terms = [product(r, b, slice(None), 1) for r, b in pair]
        for (r, b), t in zip(pair, terms):
            at = pl.ds(b * BC, BC)
            if r == 2:
                fsend[:, at] = t.astype(bf16)
            elif r == 1:
                rsend[B, at] = t[top:].astype(bf16)
                sterm[A, at] = t[:top]
            elif r == 3:
                lsend[A, at] = t[:top].astype(bf16)
                sterm[B, at] = t[top:]
            else:
                oterm[:, at] = t

    def exchange(plan):
        def go(src, dst, which, device):
            remote(src, dst, sent, arrived.at[which], device).start()

        def out_piece(owner, b, part):
            return out.at[part, columns(owner, *batches[b])]

        def step(kind, b):
            if kind == "c":
                compute(b)
            elif kind == "F":
                for part, device in sides:
                    go(fsend.at[part, cols[b]], frecv.at[part, cols[b]], b, device)
            elif kind == "O":
                go(rsend.at[B, cols[b]], beside.at[0, B, cols[b]], nbatch + b, to_right)
                go(lsend.at[A, cols[b]], beside.at[1, A, cols[b]], nbatch + b, to_left)
            elif kind == "S":
                wait(frecv.at[:, cols[b]], arrived.at[b])
                total = (sterm[:, cols[b]] + frecv[:, cols[b]].astype(f32)).astype(bf16)
                rsend[A, cols[b]] = total[:top]
                lsend[B, cols[b]] = total[top:]
                go(rsend.at[A, cols[b]], beside.at[0, A, cols[b]], nbatch + b, to_right)
                go(lsend.at[B, cols[b]], beside.at[1, B, cols[b]], nbatch + b, to_left)
            elif kind == "P":
                wait(beside.at[:, :, cols[b]], arrived.at[nbatch + b])
                total = oterm[:, cols[b]] + beside[0, :, cols[b]].astype(f32) + beside[1, :, cols[b]].astype(f32)
                out[:, columns(0, *batches[b])] = total.astype(bf16)
                for part, device in sides:
                    go(out_piece(0, b, part), out_piece(0, b, part), 2 * nbatch + b, device)
            elif kind == "Q":
                for part, device in others:
                    go(out_piece(0, b, part), out_piece(0, b, part), 3 * nbatch, device)
            else:
                wait(frecv.at[:, cols[b]], arrived.at[2 * nbatch + b])
                for (part, device), owner in zip(sides, (tp - 1, 1)):
                    go(out_piece(owner, b, part), out_piece(owner, b, part), 3 * nbatch, device)

        for word in plan:
            with jax.named_scope(word):
                step(word[0], int(word[1:]))

    def run(first, plan):
        hidden(first, list(pending))
        exchange(plan)

    pl.when(core == 0)(lambda: run(FIRST0, PLAN0))
    pl.when(core == 1)(lambda: run(FIRST1, PLAN1))
    with jax.named_scope("last"):
        wait(beside, arrived.at[3 * nbatch])
    with jax.named_scope("drain"):
        x_remote.wait_send()
        wait(hsend, far.at[2])
        wait(wd.at[0, pl.ds(0, 6 * rows)], sent)


def solution(mesh):
    tp = mesh.shape["tp"]

    def step(x, w_gate, w_up, w_down):
        rows, depth = x.shape
        units = w_gate.shape[1]
        nj = units // 2 // BN
        chunk = depth // tp
        bf16, f32 = jnp.bfloat16, jnp.float32
        quarter = pltpu.VMEM((rows, chunk), bf16)
        dma = pltpu.SemaphoreType.DMA
        operands = [pltpu.with_memory_space_constraint(a, pltpu.HBM) for a in (x, w_gate, w_up, w_down)]
        return pl.pallas_call(
            functools.partial(kernel, tp),
            out_shape=jax.ShapeDtypeStruct((rows, depth), bf16),
            in_specs=[pl.BlockSpec(memory_space=pltpu.HBM)] * 4,
            out_specs=pl.BlockSpec(memory_space=pltpu.VMEM),
            scratch_shapes=[
                pltpu.VMEM((2, rows, depth), bf16),
                pltpu.VMEM((nj, 2, depth, BN), bf16),
                pltpu.VMEM((tp, units, chunk), bf16),
                pltpu.VMEM((rows, units), bf16),
                pltpu.VMEM((rows, units // 2), bf16),
                quarter, quarter, quarter, quarter,
                pltpu.VMEM((2, rows, chunk), bf16),
                pltpu.VMEM((rows, chunk), f32),
                pltpu.VMEM((rows, chunk), f32),
                dma((nj + 1,)), dma((5,)), dma((4,)), dma((3 * len(BATCHES) + 1,)), dma,
            ],
            compiler_params=pltpu.CompilerParams(
                collective_id=0, has_side_effects=True, vmem_limit_bytes=40 * 2**20
            ),
        )(*operands)

    return jax.shard_map(
        step,
        mesh=mesh,
        in_specs=(P("dp", None), P(None, "tp"), P(None, "tp"), P("tp", None)),
        out_specs=P("dp", None),
        check_vma=False,
    )
```

```python
import functools

import jax
import jax.numpy as jnp
from jax import lax
from jax.experimental import pallas as pl
from jax.experimental.pallas import tpu as pltpu
from jax.sharding import PartitionSpec as P

MESH = pl.DeviceIdType.MESH
BN = 256
BC = 256
UNIT = 128
BATCHES = ((0, 1), (1, 1), (2, 1), (3, 1), (4, 2))
FIRST0 = ('g0', 'r4', 'm0', 'x0', 'p0', 'g1', 'r2', 'm1p1', 'g2', 'r1', 'p2', 'h0', 'h1', 'h2', 'g3', 'p3', 'h3', 'r1', 'm2m3')
FIRST1 = ('g0', 'r4', 'm0', 'g1', 'x0', 'r2', 'm1p0', 'g2', 'r1', 'p1p2', 'h0', 'h1', 'h2', 'g3', 'p3', 'h3', 'r1', 'm2m3')
PLAN0 = ('c0', 'F0', 'F1', 'c1', 'F2', 'F4', 'F3', 'c2', 'c3', 'c4', 'O2', 'O0', 'O4', 'c5', 'S0', 'S2', 'S4', 'S1', 'O1', 'S3', 'O3', 'P0', 'P2', 'Q2', 'P4', 'P1', 'Q0', 'P3', 'Q3', 'Q4', 'H2', 'Q1', 'H4', 'H0', 'H1', 'H3')
PLAN1 = ('c0', 'F1', 'F0', 'c1', 'c2', 'F2', 'F4', 'c3', 'O2', 'F3', 'O1', 'S1', 'c4', 'O0', 'O3', 'S0', 'c5', 'S2', 'P1', 'S4', 'O4', 'S3', 'Q1', 'P0', 'P2', 'Q0', 'P4', 'P3', 'Q4', 'Q2', 'H0', 'H1', 'H2', 'Q3', 'H4', 'H3')


def kernel(
    tp,
    x_hbm, wg_hbm, wu_hbm, wd_hbm,
    out,
    xs, wgu, wd, hid, hsend, fsend, frecv, rsend, lsend, beside, sterm, oterm,
    reads, downs, far, arrived, sent,
):
    rows, depth = x_hbm.shape
    top = rows // 2
    nj = wgu.shape[0]
    fh = nj * BN
    chunk = depth // tp
    nb = chunk // BC
    nbatch = len(BATCHES)
    bf16, f32 = jnp.bfloat16, jnp.float32

    me = lax.axis_index("tp")
    dp = lax.axis_index("dp")
    core = lax.rem(dp, 2)
    partner = dp + 1 - 2 * core
    right, left = lax.rem(me + 1, tp), lax.rem(me + tp - 1, tp)
    to_right, to_left, to_partner = {"tp": right}, {"tp": left}, {"dp": partner}

    barrier = pltpu.get_barrier_semaphore()
    even = lax.rem(me, 2) == 0

    def greet(*devices):
        for device in devices:
            pl.semaphore_signal(barrier, inc=1, device_id=device, device_id_type=MESH)

    greet(to_partner)

    def remote(src, dst, send, recv, device):
        return pltpu.make_async_remote_copy(
            src_ref=src, dst_ref=dst, send_sem=send, recv_sem=recv, device_id=device, device_id_type=MESH
        )

    def wait(ref, sem):
        pltpu.make_async_copy(ref, ref, sem).wait()

    def units(j):
        return pl.ds(pl.multiple_of(core * fh + j * BN, BN), BN)

    def columns(r, start, size):
        return pl.ds(pl.multiple_of(lax.rem(me + r, tp) * chunk + start, UNIT), size)

    pending = [pltpu.make_async_copy(x_hbm, xs.at[0], reads.at[nj])]
    for j in range(nj):
        for i, w in enumerate((wg_hbm, wu_hbm)):
            pending.append(pltpu.make_async_copy(w.at[:, units(j)], wgu.at[j, i], reads.at[j]))
    downs_of = ((2, 0, 2 * BC), (2, 2 * BC, chunk - 2 * BC), (1, 0, chunk), (3, 0, chunk), (0, 0, chunk))
    for i, (r, start, size) in enumerate(downs_of):
        pending.append(
            pltpu.make_async_copy(wd_hbm.at[:, columns(r, start, size)], wd.at[r, :, pl.ds(start, size)], downs.at[i])
        )
    down_copies = pending[-len(downs_of) :]

    def start_reads(count):
        for _ in range(count):
            pending.pop(0).start()

    start_reads(3)
    with jax.named_scope("barrier"):
        pl.when(even)(lambda: pl.semaphore_wait(barrier, 1))
        pl.when(jnp.logical_not(even))(lambda: pl.semaphore_wait(barrier, 3))
        greet(to_right, to_left)
    with jax.named_scope("x_wait"):
        wait(xs.at[0], reads.at[nj])
        start_reads(2)
    x_remote = remote(xs.at[0], xs.at[1], far.at[0], far.at[1], to_partner)
    x_remote.start()

    def block(j, other):
        x = xs[1 if other else 0]
        gate = jnp.dot(x, wgu[j, 0], preferred_element_type=f32)
        up = jnp.dot(x, wgu[j, 1], preferred_element_type=f32)
        h = (jax.nn.silu(gate) * up).astype(bf16)
        if other:
            hsend[:, pl.ds(j * BN, BN)] = h
        else:
            hid[:, units(j)] = h

    def hidden(plan, later):
        for word in plan:
            with jax.named_scope(word):
                kind, j = word[0], int(word[1])
                if kind == "g":
                    wait(wgu.at[j], reads.at[j])
                elif kind == "x":
                    x_remote.wait_recv()
                elif kind == "h":
                    remote(
                        hsend.at[:, pl.ds(j * BN, BN)], hid.at[:, units(j)], far.at[2], far.at[3], to_partner
                    ).start()
                elif kind == "r":
                    for _ in range(j):
                        later.pop(0).start()
                else:
                    for i in range(0, len(word), 2):
                        block(int(word[i + 1]), word[i] == "p")
        with jax.named_scope("hidden_remote"):
            wait(hid.at[:, pl.ds(pl.multiple_of((1 - core) * fh, fh), fh)], far.at[3])
            pl.when(even)(lambda: pl.semaphore_wait(barrier, 2))

    A, B = pl.ds(0, top), pl.ds(top, top)
    sides = ((A, to_right), (B, to_left))
    others = ((B, to_right), (A, to_left))
    batches = [(UNIT * a, UNIT * n) for a, n in BATCHES]
    cols = [pl.ds(start, size) for start, size in batches]
    steps = [[(2, 0)], [(2, b) for b in range(1, nb)]] + [[(1, b), (3, b)] for b in range(nb)] + [[(0, b) for b in range(nb)]]
    needs = {(2, 0): 0, (2, 2): 1, (1, 0): 2, (3, 0): 3, (0, 0): 4}

    def compute(i):
        pair = steps[i]
        for key in pair:
            if key in needs:
                down_copies[needs[key]].wait()
                if needs[key] == 0:
                    down_copies[4].start()
        def product(r, b, half, sign):
            return jnp.dot(sign * hid[:, half], wd[r, half, pl.ds(b * BC, BC)], preferred_element_type=f32)

        if len(pair) == 1:
            terms = [product(*pair[0], pl.ds(0, fh), 1) - product(*pair[0], pl.ds(fh, fh), -1)]
        else:
            terms = [product(r, b, slice(None), 1) for r, b in pair]
        for (r, b), t in zip(pair, terms):
            at = pl.ds(b * BC, BC)
            if r == 2:
                fsend[:, at] = t.astype(bf16)
            elif r == 1:
                rsend[B, at] = t[top:].astype(bf16)
                sterm[A, at] = t[:top]
            elif r == 3:
                lsend[A, at] = t[:top].astype(bf16)
                sterm[B, at] = t[top:]
            else:
                oterm[:, at] = t

    def exchange(plan):
        def go(src, dst, which, device):
            remote(src, dst, sent, arrived.at[which], device).start()

        def out_piece(owner, b, part):
            return out.at[part, columns(owner, *batches[b])]

        def step(kind, b):
            if kind == "c":
                compute(b)
            elif kind == "F":
                for part, device in sides:
                    go(fsend.at[part, cols[b]], frecv.at[part, cols[b]], b, device)
            elif kind == "O":
                go(rsend.at[B, cols[b]], beside.at[0, B, cols[b]], nbatch + b, to_right)
                go(lsend.at[A, cols[b]], beside.at[1, A, cols[b]], nbatch + b, to_left)
            elif kind == "S":
                wait(frecv.at[:, cols[b]], arrived.at[b])
                total = (sterm[:, cols[b]] + frecv[:, cols[b]].astype(f32)).astype(bf16)
                rsend[A, cols[b]] = total[:top]
                lsend[B, cols[b]] = total[top:]
                go(rsend.at[A, cols[b]], beside.at[0, A, cols[b]], nbatch + b, to_right)
                go(lsend.at[B, cols[b]], beside.at[1, B, cols[b]], nbatch + b, to_left)
            elif kind == "P":
                wait(beside.at[:, :, cols[b]], arrived.at[nbatch + b])
                total = oterm[:, cols[b]] + beside[0, :, cols[b]].astype(f32) + beside[1, :, cols[b]].astype(f32)
                out[:, columns(0, *batches[b])] = total.astype(bf16)
                for part, device in sides:
                    go(out_piece(0, b, part), out_piece(0, b, part), 2 * nbatch + b, device)
            elif kind == "Q":
                for part, device in others:
                    go(out_piece(0, b, part), out_piece(0, b, part), 3 * nbatch, device)
            else:
                wait(frecv.at[:, cols[b]], arrived.at[2 * nbatch + b])
                for (part, device), owner in zip(sides, (tp - 1, 1)):
                    go(out_piece(owner, b, part), out_piece(owner, b, part), 3 * nbatch, device)

        for word in plan:
            with jax.named_scope(word):
                step(word[0], int(word[1:]))

    def run(first, plan):
        hidden(first, list(pending))
        exchange(plan)

    pl.when(core == 0)(lambda: run(FIRST0, PLAN0))
    pl.when(core == 1)(lambda: run(FIRST1, PLAN1))
    with jax.named_scope("last"):
        wait(beside, arrived.at[3 * nbatch])
    with jax.named_scope("drain"):
        x_remote.wait_send()
        wait(hsend, far.at[2])
        wait(wd.at[0, pl.ds(0, 6 * rows)], sent)


def solution(mesh):
    tp = mesh.shape["tp"]

    def step(x, w_gate, w_up, w_down):
        rows, depth = x.shape
        units = w_gate.shape[1]
        nj = units // 2 // BN
        chunk = depth // tp
        bf16, f32 = jnp.bfloat16, jnp.float32
        quarter = pltpu.VMEM((rows, chunk), bf16)
        dma = pltpu.SemaphoreType.DMA
        operands = [pltpu.with_memory_space_constraint(a, pltpu.HBM) for a in (x, w_gate, w_up, w_down)]
        return pl.pallas_call(
            functools.partial(kernel, tp),
            out_shape=jax.ShapeDtypeStruct((rows, depth), bf16),
            in_specs=[pl.BlockSpec(memory_space=pltpu.HBM)] * 4,
            out_specs=pl.BlockSpec(memory_space=pltpu.VMEM),
            scratch_shapes=[
                pltpu.VMEM((2, rows, depth), bf16),
                pltpu.VMEM((nj, 2, depth, BN), bf16),
                pltpu.VMEM((tp, units, chunk), bf16),
                pltpu.VMEM((rows, units), bf16),
                pltpu.VMEM((rows, units // 2), bf16),
                quarter, quarter, quarter, quarter,
                pltpu.VMEM((2, rows, chunk), bf16),
                pltpu.VMEM((rows, chunk), f32),
                pltpu.VMEM((rows, chunk), f32),
                dma((nj + 1,)), dma((5,)), dma((4,)), dma((3 * len(BATCHES) + 1,)), dma,
            ],
            compiler_params=pltpu.CompilerParams(
                collective_id=0, has_side_effects=True, vmem_limit_bytes=40 * 2**20
            ),
        )(*operands)

    return jax.shard_map(
        step,
        mesh=mesh,
        in_specs=(P("dp", None), P(None, "tp"), P(None, "tp"), P("tp", None)),
        out_specs=P("dp", None),
        check_vma=False,
    )
```
